32 devices in a mesh: ez: 4 (over z), ey: 2 (over y), ex: 4 (over x, core).
Axes of the slice: x: 2, y: 2, z: 4, core: 2. Of those that a mesh axis runs over, the one named last changes fastest.
Arguments:
- tokens: bfloat16 [8192, 2560], P(('ez', 'ey', 'ex'))
- expert_ids: int32 [8192, 6], P(('ez', 'ey', 'ex'))
- gate_weights: float32 [8192, 6], P(('ez', 'ey', 'ex'))
- w_gate: bfloat16 [64, 2560, 1536], P(('ez', 'ey', 'ex'))
- w_up: bfloat16 [64, 2560, 1536], P(('ez', 'ey', 'ex'))
- w_down: bfloat16 [64, 1536, 2560], P(('ez', 'ey', 'ex'))
Outputs:
- output: bfloat16 [8192, 2560], P(('ez', 'ey', 'ex'))
All inputs are finite; a program needn't handle non-finite values.
Results may differ from the reference program's by a relative error of at most 0.00615969.
Values are sent between devices in bfloat16 or wider.
A program may use at most 1 GiB of HBM per device.

```python
import jax
import jax.numpy as jnp
from jax import lax

HIDDEN = 2560
EXPERT_FF = 1536
EXPERTS = 64
TOP_K = 6
TOKENS = 256
DEVICES = 32
TOTAL_TOK = DEVICES * TOKENS
LOCAL_EXPERTS = EXPERTS // DEVICES
PER_EXPERT = TOTAL_TOK * TOP_K // EXPERTS


def draw_routing(route_key):
    def one_source(src_key):
        key_first, key_rest, key_dev, key_order = jax.random.split(src_key, 4)
        first_block = jax.random.permutation(key_first, LOCAL_EXPERTS)
        rest_block = jax.random.permutation(key_rest, EXPERTS - LOCAL_EXPERTS) + LOCAL_EXPERTS
        positions = jnp.arange(EXPERTS)
        spaced = positions % DEVICES == 0
        first_idx = jnp.clip(positions // DEVICES, 0, LOCAL_EXPERTS - 1)
        rest_idx = jnp.clip(positions - positions // DEVICES - 1, 0, EXPERTS - LOCAL_EXPERTS - 1)
        expert_cycle = jnp.where(spaced, first_block[first_idx], rest_block[rest_idx])
        dev_perm = jax.random.permutation(key_dev, DEVICES)
        expert_cycle = dev_perm[expert_cycle // LOCAL_EXPERTS] * LOCAL_EXPERTS + expert_cycle % LOCAL_EXPERTS
        tok_perm = jax.random.permutation(key_order, TOKENS)
        slot_pos = tok_perm[:, None] * TOP_K + jnp.arange(TOP_K)[None, :]
        return expert_cycle[slot_pos % EXPERTS]
    src_keys = jax.random.split(route_key, DEVICES)
    return jax.vmap(one_source)(src_keys).reshape(TOTAL_TOK, TOP_K).astype(jnp.int32)


def setup_inputs(seed: int = 0) -> dict:
    root_key = jax.random.key(seed)
    key_tok, key_ids, key_gate, key_w1, key_w3, key_w2 = jax.random.split(root_key, 6)
    tokens = jax.random.normal(key_tok, (TOTAL_TOK, HIDDEN), jnp.float32).astype(jnp.bfloat16)
    expert_ids = draw_routing(key_ids)
    gate_logits = 0.7 * jax.random.normal(key_gate, (TOTAL_TOK, TOP_K), jnp.float32)
    gate_weights = jax.nn.softmax(gate_logits, axis=-1)
    w_gate = (jax.random.normal(key_w1, (EXPERTS, HIDDEN, EXPERT_FF), jnp.float32) * HIDDEN ** -0.5).astype(jnp.bfloat16)
    w_up = (jax.random.normal(key_w3, (EXPERTS, HIDDEN, EXPERT_FF), jnp.float32) * HIDDEN ** -0.5).astype(jnp.bfloat16)
    w_down = (jax.random.normal(key_w2, (EXPERTS, EXPERT_FF, HIDDEN), jnp.float32) * (2.0 * EXPERT_FF ** -0.5)).astype(jnp.bfloat16)
    return {"tokens": tokens, "expert_ids": expert_ids, "gate_weights": gate_weights, "w_gate": w_gate, "w_up": w_up, "w_down": w_down}


def reference(tokens, expert_ids, gate_weights, w_gate, w_up, w_down):
    sort_order = jnp.argsort(expert_ids.reshape(-1), stable=True)
    rows_by_expert = (sort_order // TOP_K).reshape(EXPERTS, PER_EXPERT)
    gates_by_expert = gate_weights.reshape(-1)[sort_order].reshape(EXPERTS, PER_EXPERT)

    def expert_step(acc_out, expert_args):
        row_ids, row_gates, gate_mat, up_mat, down_mat = expert_args
        x_rows = tokens[row_ids]
        gate_act = jnp.dot(x_rows, gate_mat, preferred_element_type=jnp.float32)
        up_act = jnp.dot(x_rows, up_mat, preferred_element_type=jnp.float32)
        hidden_act = (jax.nn.silu(gate_act) * up_act).astype(jnp.bfloat16)
        expert_out = jnp.dot(hidden_act, down_mat, preferred_element_type=jnp.float32)
        acc_out = acc_out.at[row_ids].add(expert_out * row_gates[:, None])
        return acc_out, None

    init_acc = jnp.zeros((TOTAL_TOK, HIDDEN), jnp.float32)
    moe_sum = lax.scan(expert_step, init_acc, (rows_by_expert, gates_by_expert, w_gate, w_up, w_down))[0]
    return (tokens.astype(jnp.float32) + moe_sum).astype(jnp.bfloat16)
```

```python
import functools
import math
import jax
import jax.numpy as jnp
from jax import lax
from jax.experimental import pallas as pl
from jax.experimental.pallas import tpu as pltpu
from jax.sharding import PartitionSpec as P

BF = jnp.bfloat16
F32 = jnp.float32
MESH = pl.DeviceIdType.MESH
TAIL = 128
PLANE = 8
ZED = 4
SLICES = 4


def layer_kernel(dims, x_ref, tail_ref, w1_ref, w3_ref, w2_ref, y_ref,
                 zbuf, send, recv, back, hid, zsend, zrecv, unpack, wa, wb,
                 x_sem, wa_sem, wb_sem, z_ssem, z_rsem, d_ssem, d_rsem,
                 b_ssem, b_rsem, s_ssem, s_rsem):
    tok, wide, ff, cap, ft, nt = dims
    rows = PLANE * cap
    full = wide + TAIL
    sw = wide // SLICES
    n_f, n_n = ff // ft, wide // nt
    z = lax.axis_index("ez")
    ey = lax.axis_index("ey")
    ex = lax.axis_index("ex")
    me = ey * 4 + ex
    mid = jnp.logical_and(z > 0, z < 3)
    end = jnp.logical_or(z < 1, z > 2)

    def peer(o):
        cy = ey if o < 4 else 1 - ey
        cx = (ex, ex + 1 - 2 * (ex % 2), (ex + 2) % 4, 3 - ex)[o % 4]
        return cy, cx

    def rows_of(q):
        return pl.ds(pl.multiple_of(q * cap, cap), cap)

    src_z = (z, z + 1 - 2 * (z % 2), 2 - z // 2, 3 - 3 * (z // 2))
    order = (6, 4, 2, 7, 5, 3, 1)

    barrier = pltpu.get_barrier_semaphore()
    for o in range(1, PLANE):
        cy, cx = peer(o)
        pl.semaphore_signal(barrier, inc=1, device_id=(z, cy, cx), device_id_type=MESH)

    @pl.when(z > 0)
    def _():
        pl.semaphore_signal(barrier, inc=1, device_id=(z - 1, ey, ex), device_id_type=MESH)

    @pl.when(z < 3)
    def _():
        pl.semaphore_signal(barrier, inc=1, device_id=(z + 1, ey, ex), device_id_type=MESH)

    own = pltpu.make_async_copy(x_ref, zbuf.at[z, :, pl.ds(0, wide)], x_sem.at[0])
    own.start()
    zbuf[z, :, wide:] = tail_ref[...]

    def a_copies(i):
        l, f, slot = i // n_f, i % n_f, i % 2
        cols = pl.ds(pl.multiple_of(f * ft, ft), ft)
        return [pltpu.make_async_copy(w.at[l, :, cols], wa.at[slot, j], wa_sem.at[slot, j])
                for j, w in enumerate((w1_ref, w3_ref))]

    def b_copies(n):
        slot = n % 2
        cols = pl.ds(pl.multiple_of(n * nt, nt), nt)
        return [pltpu.make_async_copy(w2_ref.at[l, :, cols], wb.at[slot, l], wb_sem.at[slot, l])
                for l in range(2)]

    for c in a_copies(0):
        c.start()
    own.wait()
    pl.semaphore_wait(barrier, PLANE - 1 + jnp.where(mid, 2, 1))

    def z_copy(block, target, i):
        return pltpu.make_async_remote_copy(
            src_ref=zbuf.at[block], dst_ref=zbuf.at[block],
            send_sem=z_ssem.at[i], recv_sem=z_rsem.at[block],
            device_id=(target, ey, ex), device_id_type=MESH)

    @pl.when(z > 0)
    def _():
        z_copy(z, z - 1, 0).start()

    @pl.when(z < 3)
    def _():
        z_copy(z, z + 1, 1).start()

    def fwd_copy(k):
        return z_copy(src_z[k], 3 - z if k == 1 else 3 * (z - 1), 1 + k)

    def z_wait(k):
        z_copy(src_z[k], z, 0).wait_recv()

    def d_copy(k, o):
        cy, cx = peer(o)
        return pltpu.make_async_remote_copy(
            src_ref=send.at[k, rows_of(cy * 4 + cx)], dst_ref=recv.at[k, rows_of(me)],
            send_sem=d_ssem.at[k, o], recv_sem=d_rsem.at[k, o],
            device_id=(z, cy, cx), device_id_type=MESH)

    def relay(k):
        b = src_z[k]
        tail = zbuf[b, :, wide:].astype(F32)
        lane = lax.broadcasted_iota(jnp.int32, (tok, TAIL), 1)
        want_dev = jnp.where(lane < PLANE, z * PLANE + lane, -2).astype(F32)
        want_exp = jnp.where(lane < 48, z * 16 + jnp.bitwise_and(lane, 15), -2).astype(F32)
        hit = jnp.zeros((tok, TAIL), F32)
        gates = jnp.zeros((tok, TAIL), F32)
        for j in range(6):
            hit = jnp.where(tail[:, j:j + 1] == want_dev, 1.0, hit)
            part = jnp.where(lane < 16, tail[:, 16 + j:17 + j],
                             jnp.where(lane < 32, tail[:, 24 + j:25 + j], tail[:, 32 + j:33 + j]))
            gates = jnp.where(tail[:, 8 + j:9 + j] == want_exp, part, gates)
        r_i = lax.broadcasted_iota(jnp.int32, (tok, tok), 0)
        c_i = lax.broadcasted_iota(jnp.int32, (tok, tok), 1)
        tri = jnp.where(c_i <= r_i, 1.0, 0.0).astype(BF)
        rank = jnp.dot(tri, hit.astype(BF), preferred_element_type=F32)
        pos = jnp.where(hit > 0.0, rank, 0.0).astype(BF)
        d_i = lax.broadcasted_iota(jnp.int32, (TAIL, rows), 0)
        s_i = lax.broadcasted_iota(jnp.int32, (TAIL, rows), 1)
        spread = jnp.where(jnp.logical_and(s_i >= d_i * cap, s_i < d_i * cap + cap), 1.0, 0.0).astype(BF)
        l_i = lax.broadcasted_iota(jnp.int32, (tok, rows), 1)
        slot_l = l_i + 1
        for q in range(1, PLANE):
            slot_l = slot_l - jnp.where(l_i >= q * cap, cap, 0)
        at_l = jnp.dot(pos, spread, preferred_element_type=F32)
        unpack[k] = jnp.where(at_l == slot_l.astype(F32), 1.0, 0.0).astype(BF)
        d_t = lax.broadcasted_iota(jnp.int32, (rows, TAIL), 1)
        s_t = lax.broadcasted_iota(jnp.int32, (rows, TAIL), 0)
        spread_t = jnp.where(jnp.logical_and(s_t >= d_t * cap, s_t < d_t * cap + cap), 1.0, 0.0).astype(BF)
        r_t = lax.broadcasted_iota(jnp.int32, (rows, tok), 0)
        slot_r = r_t + 1
        for q in range(1, PLANE):
            slot_r = slot_r - jnp.where(r_t >= q * cap, cap, 0)
        at_r = lax.dot_general(spread_t, pos, (((1,), (1,)), ((), ())), preferred_element_type=F32)
        pick = jnp.where(at_r == slot_r.astype(F32), 1.0, 0.0).astype(BF)
        for s in range(SLICES):
            cols = slice(s * sw, s * sw + sw)
            send[k, :, cols] = jnp.dot(pick, zbuf[b, :, cols], preferred_element_type=F32).astype(BF)
        send[k, :, wide:] = jnp.dot(pick, gates.astype(BF), preferred_element_type=F32).astype(BF)
        for o in order:
            d_copy(k, o).start()
        recv[k, rows_of(me), :] = send[k, rows_of(me), :]

    def service(k):
        z_wait(k)
        relay(k)

    def forward(k):
        @pl.when(mid)
        def _():
            fwd_copy(k).start()

    def arrive(k):
        for o in order:
            d_copy(k, o).wait_recv()

    def stage_a(k, l):
        def step(i, carry):
            @pl.when(i + 1 < 2 * n_f)
            def _():
                for c in a_copies(i + 1):
                    c.start()

            @pl.when(i + 1 == 2 * n_f)
            def _():
                for c in b_copies(0):
                    c.start()
            for c in a_copies(i):
                c.wait()
            slot = i % 2
            x = recv[k, :, :wide]
            a = jnp.dot(x, wa[slot, 0], preferred_element_type=F32)
            b = jnp.dot(x, wa[slot, 1], preferred_element_type=F32)
            cols = pl.ds(pl.multiple_of((i - l * n_f) * ft, ft), ft)
            hid[l, :, cols] = (jax.nn.silu(a) * b).astype(BF)
            return carry
        lax.fori_loop(l * n_f, (l + 1) * n_f, step, 0)

    def stage_b(k):
        tail = recv[k, :, wide:].astype(F32)
        lane = lax.broadcasted_iota(jnp.int32, (rows, TAIL), 1)
        gate = []
        for l in range(2):
            at = jnp.where(lane < 48, jnp.bitwise_and(lane, 15), -1) == me * 2 + l
            gate.append(jnp.sum(jnp.where(at, tail, 0.0), axis=1, keepdims=True))

        def step(n, carry):
            @pl.when(n + 1 < n_n)
            def _():
                for c in b_copies(n + 1):
                    c.start()
            if k < ZED - 1:
                @pl.when(n + 1 == n_n)
                def _():
                    for c in a_copies(0):
                        c.start()
            for c in b_copies(n):
                c.wait()
            slot = n % 2
            o0 = jnp.dot(hid[0], wb[slot, 0], preferred_element_type=F32)
            o1 = jnp.dot(hid[1], wb[slot, 1], preferred_element_type=F32)
            cols = pl.ds(pl.multiple_of(n * nt, nt), nt)
            recv[k, :, cols] = (gate[0] * o0 + gate[1] * o1).astype(BF)
            return carry
        lax.fori_loop(0, n_n, step, 0)

    def b_copy(k, o):
        cy, cx = peer(o)
        return pltpu.make_async_remote_copy(
            src_ref=recv.at[k, rows_of(cy * 4 + cx), pl.ds(0, wide)], dst_ref=back.at[k, rows_of(me)],
            send_sem=b_ssem.at[k, o], recv_sem=b_rsem.at[k, o],
            device_id=(z, cy, cx), device_id_type=MESH)

    def give_back(k):
        for o in order:
            b_copy(k, o).start()
        back[k, rows_of(me), :] = recv[k, rows_of(me), :wide]

    def back_wait(k):
        for o in order:
            b_copy(k, o).wait_recv()

    def s_copy(k, s):
        if k == 1:
            target, slot = src_z[1], jnp.where(z % 2 == 0, z + 1, 4)
        elif k == 2:
            target = z + 1 - 2 * (z // 2)
            slot = jnp.where(z < 2, 2, jnp.where(z == 2, 4, 1))
        else:
            target, slot = z + 1 - 2 * (z // 2), src_z[3]
        cols = pl.ds(s * sw, sw)
        return pltpu.make_async_remote_copy(
            src_ref=zsend.at[k - 1, :, cols], dst_ref=zrecv.at[slot, :, cols],
            send_sem=s_ssem.at[k - 1, s], recv_sem=s_rsem.at[slot, s],
            device_id=(target, ey, ex), device_id_type=MESH)

    def s_wait(slot, s):
        cols = pl.ds(s * sw, sw)
        pltpu.make_async_remote_copy(
            src_ref=zsend.at[0, :, cols], dst_ref=zrecv.at[slot, :, cols],
            send_sem=s_ssem.at[0, s], recv_sem=s_rsem.at[slot, s],
            device_id=(z, ey, ex), device_id_type=MESH).wait_recv()

    def partial(k, s):
        return jnp.dot(unpack[k], back[k, :, s * sw:s * sw + sw], preferred_element_type=F32)

    def finish_end(k):
        for s in range(SLICES):
            zsend[k - 1, :, s * sw:s * sw + sw] = partial(k, s).astype(BF)
            s_copy(k, s).start()

    def finish_mid(k):
        for s in range(SLICES):
            cols = slice(s * sw, s * sw + sw)
            s_wait(src_z[k], s)
            total = partial(k, s) + zrecv[src_z[k], :, cols].astype(F32)
            zsend[k - 1, :, cols] = total.astype(BF)
            s_copy(k, s).start()

    def finish(k):
        back_wait(k)
        pl.when(end)(lambda: finish_end(k))
        pl.when(mid)(lambda: finish_mid(k))

    relay(0)
    arrive(0)
    stage_a(0, 0)
    z_wait(1)
    forward(1)

    @pl.when(mid)
    def _():
        z_wait(2)
        fwd_copy(2).start()
    relay(1)
    stage_a(0, 1)
    stage_b(0)

    arrive(1)
    stage_a(1, 0)

    @pl.when(end)
    def _():
        z_wait(2)
    relay(2)

    @pl.when(mid)
    def _():
        z_wait(3)
        fwd_copy(3).start()
    stage_a(1, 1)
    stage_b(1)
    give_back(1)

    arrive(2)
    stage_a(2, 0)

    @pl.when(end)
    def _():
        z_wait(3)
    relay(3)
    stage_a(2, 1)
    stage_b(2)
    give_back(2)

    @pl.when(end)
    def _():
        back_wait(1)
        finish_end(1)
    arrive(3)
    stage_a(3, 0)
    stage_a(3, 1)
    stage_b(3)
    give_back(3)
    give_back(0)
    finish(2)
    finish(3)

    @pl.when(mid)
    def _():
        back_wait(1)
        finish_mid(1)
    back_wait(0)

    for s in range(SLICES):
        cols = slice(s * sw, s * sw + sw)

        @pl.when(z > 0)
        def _():
            s_wait(z, s)

        @pl.when(z < 3)
        def _():
            s_wait(4, s)
        total = zbuf[z, :, cols].astype(F32) + partial(0, s)

        @pl.when(z == 0)
        def _():
            y_ref[:, cols] = (total + zrecv[4, :, cols].astype(F32)).astype(BF)

        @pl.when(z == 3)
        def _():
            y_ref[:, cols] = (total + zrecv[3, :, cols].astype(F32)).astype(BF)

        @pl.when(mid)
        def _():
            both = zrecv[z, :, cols].astype(F32) + zrecv[4, :, cols].astype(F32)
            y_ref[:, cols] = (total + both).astype(BF)

    @pl.when(z > 0)
    def _():
        z_copy(z, z - 1, 0).wait_send()

    @pl.when(z < 3)
    def _():
        z_copy(z, z + 1, 1).wait_send()

    @pl.when(mid)
    def _():
        for k in range(1, ZED):
            fwd_copy(k).wait_send()
    for k in range(ZED):
        for o in order:
            d_copy(k, o).wait_send()
            b_copy(k, o).wait_send()
    for k in range(1, ZED):
        for s in range(SLICES):
            s_copy(k, s).wait_send()


def split_gates(gates):
    first = lax.reduce_precision(gates, 8, 7)
    second = lax.reduce_precision(gates - first, 8, 7)
    third = gates - first - second
    return first, second, third


def solution(mesh):
    ep_axes = tuple(mesh.axis_names)
    num_devices = math.prod(mesh.shape[a] for a in ep_axes)
    row_spec = P(ep_axes, None)
    w_spec = P(ep_axes, None, None)

    def local_layer(tokens, expert_ids, gate_weights, w_gate, w_up, w_down):
        tok, wide = tokens.shape
        ff = w_gate.shape[2]
        cap = tok * expert_ids.shape[1] // num_devices
        rows = PLANE * cap
        ft, nt = 256, 256
        full = wide + TAIL

        def eight(v):
            return jnp.pad(v.astype(F32), ((0, 0), (0, 2)), constant_values=-1.0)
        parts = [eight(expert_ids // 2), eight(expert_ids)]
        parts += [eight(g) for g in split_gates(gate_weights)]
        tail = jnp.concatenate(parts, axis=1)
        tail = jnp.pad(tail, ((0, 0), (0, TAIL - tail.shape[1]))).astype(BF)

        dims = (tok, wide, ff, cap, ft, nt)
        vm = pl.BlockSpec(memory_space=pltpu.VMEM)
        hbm = pl.BlockSpec(memory_space=pl.ANY)
        dma = pltpu.SemaphoreType.DMA
        return pl.pallas_call(
            functools.partial(layer_kernel, dims),
            out_shape=jax.ShapeDtypeStruct((tok, wide), BF),
            in_specs=[hbm, vm, hbm, hbm, hbm],
            out_specs=vm,
            scratch_shapes=[
                pltpu.VMEM((ZED, tok, full), BF),
                pltpu.VMEM((ZED, rows, full), BF),
                pltpu.VMEM((ZED, rows, full), BF),
                pltpu.VMEM((ZED, rows, wide), BF),
                pltpu.VMEM((2, rows, ff), BF),
                pltpu.VMEM((ZED - 1, tok, wide), BF),
                pltpu.VMEM((ZED + 1, tok, wide), BF),
                pltpu.VMEM((ZED, tok, rows), BF),
                pltpu.VMEM((2, 2, wide, ft), BF),
                pltpu.VMEM((2, 2, ff, nt), BF),
                dma((1,)), dma((2, 2)), dma((2, 2)),
                dma((5,)), dma((ZED,)),
                dma((ZED, PLANE)), dma((ZED, PLANE)),
                dma((ZED, PLANE)), dma((ZED, PLANE)),
                dma((ZED - 1, SLICES)), dma((ZED + 1, SLICES)),
            ],
            compiler_params=pltpu.CompilerParams(
                collective_id=0, has_side_effects=True, vmem_limit_bytes=67_000_000),
            name="moe_layer",
        )(tokens, tail, w_gate, w_up, w_down)

    return jax.shard_map(local_layer, mesh=mesh, in_specs=(row_spec, row_spec, row_spec, w_spec, w_spec, w_spec), out_specs=row_spec, check_vma=False)
```

```python
import functools
import math
import jax
import jax.numpy as jnp
from jax import lax
from jax.experimental import pallas as pl
from jax.experimental.pallas import tpu as pltpu
from jax.sharding import PartitionSpec as P

BF = jnp.bfloat16
F32 = jnp.float32
MESH = pl.DeviceIdType.MESH
TAIL = 128
PLANE = 8
ZED = 4
SLICES = 4
HALVES = 2
FT = 512
NT = 512


def layer_kernel(dims, x_ref, tail_ref, w1_ref, w3_ref, w2_ref, y_ref,
                 zbuf, send, recv, back, hid, gate, zsend, zrecv, unpack, wa, wb,
                 x_sem, wa_sem, wb_sem, z_ssem, z_rsem, d_ssem, d_rsem,
                 b_ssem, b_rsem, s_ssem, s_rsem):
    tok, wide, ff, cap, ft, nt = dims
    rows = PLANE * cap
    full = wide + TAIL
    sw = wide // SLICES
    hw = wide // HALVES
    per_half = SLICES // HALVES
    n_f, n_n = ff // ft, wide // nt
    z = lax.axis_index("ez")
    ey = lax.axis_index("ey")
    ex = lax.axis_index("ex")
    me = ey * 4 + ex
    mid = jnp.logical_and(z > 0, z < 3)
    end = jnp.logical_or(z < 1, z > 2)

    def peer(o):
        cy = ey if o < 4 else 1 - ey
        cx = (ex, ex + 1 - 2 * (ex % 2), (ex + 2) % 4, 3 - ex)[o % 4]
        return cy, cx

    def rows_of(q):
        return pl.ds(pl.multiple_of(q * cap, cap), cap)

    src_z = (z, z + 1 - 2 * (z % 2), 2 - z // 2, 3 - 3 * (z // 2))
    order = (6, 4, 2, 7, 5, 3, 1)

    barrier = pltpu.get_barrier_semaphore()
    for o in range(1, PLANE):
        cy, cx = peer(o)
        pl.semaphore_signal(barrier, inc=1, device_id=(z, cy, cx), device_id_type=MESH)

    @pl.when(z > 0)
    def _():
        pl.semaphore_signal(barrier, inc=1, device_id=(z - 1, ey, ex), device_id_type=MESH)

    @pl.when(z < 3)
    def _():
        pl.semaphore_signal(barrier, inc=1, device_id=(z + 1, ey, ex), device_id_type=MESH)

    own = pltpu.make_async_copy(x_ref, zbuf.at[z, :, pl.ds(0, wide)], x_sem.at[0])
    own.start()
    zbuf[z, :, wide:] = tail_ref[...]

    def a_copies(i):
        l, f, slot = i // n_f, i % n_f, i % 2
        cols = pl.ds(pl.multiple_of(f * ft, ft), ft)
        return [pltpu.make_async_copy(w.at[l, :, cols], wa.at[slot, j], wa_sem.at[slot, j])
                for j, w in enumerate((w1_ref, w3_ref))]

    def b_copies(n):
        slot = n % 2
        cols = pl.ds(pl.multiple_of(n * nt, nt), nt)
        return [pltpu.make_async_copy(w2_ref.at[l, :, cols], wb.at[slot, l], wb_sem.at[slot, l])
                for l in range(2)]

    for c in a_copies(0):
        c.start()
    own.wait()
    pl.semaphore_wait(barrier, PLANE - 1 + jnp.where(mid, 2, 1))

    def z_copy(block, target, i):
        return pltpu.make_async_remote_copy(
            src_ref=zbuf.at[block], dst_ref=zbuf.at[block],
            send_sem=z_ssem.at[i], recv_sem=z_rsem.at[block],
            device_id=(target, ey, ex), device_id_type=MESH)

    @pl.when(z > 0)
    def _():
        z_copy(z, z - 1, 0).start()

    @pl.when(z < 3)
    def _():
        z_copy(z, z + 1, 1).start()

    def fwd_copy(k):
        return z_copy(src_z[k], 3 - z if k == 1 else 3 * (z - 1), 1 + k)

    def z_wait(k):
        z_copy(src_z[k], z, 0).wait_recv()

    def d_copy(k, o):
        cy, cx = peer(o)
        return pltpu.make_async_remote_copy(
            src_ref=send.at[k, rows_of(cy * 4 + cx)], dst_ref=recv.at[k, rows_of(me)],
            send_sem=d_ssem.at[k, o], recv_sem=d_rsem.at[k, o],
            device_id=(z, cy, cx), device_id_type=MESH)

    def relay(k):
        b = src_z[k]
        tail = zbuf[b, :, wide:].astype(F32)
        lane = lax.broadcasted_iota(jnp.int32, (tok, TAIL), 1)
        want_dev = jnp.where(lane < PLANE, z * PLANE + lane, -2).astype(F32)
        want_exp = jnp.where(lane < 48, z * 16 + jnp.bitwise_and(lane, 15), -2).astype(F32)
        hit = jnp.zeros((tok, TAIL), F32)
        gates = jnp.zeros((tok, TAIL), F32)
        for j in range(6):
            hit = jnp.where(tail[:, j:j + 1] == want_dev, 1.0, hit)
            part = jnp.where(lane < 16, tail[:, 16 + j:17 + j],
                             jnp.where(lane < 32, tail[:, 24 + j:25 + j], tail[:, 32 + j:33 + j]))
            gates = jnp.where(tail[:, 8 + j:9 + j] == want_exp, part, gates)
        r_i = lax.broadcasted_iota(jnp.int32, (tok, tok), 0)
        c_i = lax.broadcasted_iota(jnp.int32, (tok, tok), 1)
        tri = jnp.where(c_i <= r_i, 1.0, 0.0).astype(BF)
        rank = jnp.dot(tri, hit.astype(BF), preferred_element_type=F32)
        pos = jnp.where(hit > 0.0, rank, 0.0).astype(BF)
        d_i = lax.broadcasted_iota(jnp.int32, (TAIL, rows), 0)
        s_i = lax.broadcasted_iota(jnp.int32, (TAIL, rows), 1)
        spread = jnp.where(jnp.logical_and(s_i >= d_i * cap, s_i < d_i * cap + cap), 1.0, 0.0).astype(BF)
        l_i = lax.broadcasted_iota(jnp.int32, (tok, rows), 1)
        slot_l = l_i + 1
        for q in range(1, PLANE):
            slot_l = slot_l - jnp.where(l_i >= q * cap, cap, 0)
        at_l = jnp.dot(pos, spread, preferred_element_type=F32)
        unpack[k] = jnp.where(at_l == slot_l.astype(F32), 1.0, 0.0).astype(BF)
        d_t = lax.broadcasted_iota(jnp.int32, (rows, TAIL), 1)
        s_t = lax.broadcasted_iota(jnp.int32, (rows, TAIL), 0)
        spread_t = jnp.where(jnp.logical_and(s_t >= d_t * cap, s_t < d_t * cap + cap), 1.0, 0.0).astype(BF)
        r_t = lax.broadcasted_iota(jnp.int32, (rows, tok), 0)
        slot_r = r_t + 1
        for q in range(1, PLANE):
            slot_r = slot_r - jnp.where(r_t >= q * cap, cap, 0)
        at_r = lax.dot_general(spread_t, pos, (((1,), (1,)), ((), ())), preferred_element_type=F32)
        pick = jnp.where(at_r == slot_r.astype(F32), 1.0, 0.0).astype(BF)
        for s in range(SLICES):
            cols = slice(s * sw, s * sw + sw)
            send[k, :, cols] = jnp.dot(pick, zbuf[b, :, cols], preferred_element_type=F32).astype(BF)
        send[k, :, wide:] = jnp.dot(pick, gates.astype(BF), preferred_element_type=F32).astype(BF)
        for o in order:
            d_copy(k, o).start()
        recv[k, rows_of(me), :] = send[k, rows_of(me), :]

    def forward(k):
        @pl.when(mid)
        def _():
            fwd_copy(k).start()

    def arrive(k):
        for o in order:
            d_copy(k, o).wait_recv()

    def step_a(k, i):
        @pl.when(i + 1 < 2 * n_f)
        def _():
            for c in a_copies(i + 1):
                c.start()

        @pl.when(i + 1 == 2 * n_f)
        def _():
            for c in b_copies(0):
                c.start()
        for c in a_copies(i):
            c.wait()
        slot = i % 2
        x = recv[k, :, :wide]
        a = jnp.dot(x, wa[slot, 0], preferred_element_type=F32)
        b = jnp.dot(x, wa[slot, 1], preferred_element_type=F32)
        cols = pl.ds(pl.multiple_of((i % n_f) * ft, ft), ft)
        hid[i // n_f, :, cols] = (jax.nn.silu(a) * b).astype(BF)

    def step_gate(k):
        tail = recv[k, :, wide:].astype(F32)
        lane = lax.broadcasted_iota(jnp.int32, (rows, TAIL), 1)
        for l in range(2):
            at = jnp.where(lane < 48, jnp.bitwise_and(lane, 15), -1) == me * 2 + l
            g = jnp.sum(jnp.where(at, tail, 0.0), axis=1, keepdims=True)
            gate[l] = jnp.broadcast_to(g, (rows, TAIL))

    def step_b(k, n):
        @pl.when(n + 1 < n_n)
        def _():
            for c in b_copies(n + 1):
                c.start()

        @pl.when(jnp.logical_and(n + 1 == n_n, k < ZED - 1))
        def _():
            for c in a_copies(0):
                c.start()
        for c in b_copies(n):
            c.wait()
        slot = n % 2
        o0 = jnp.dot(hid[0], wb[slot, 0], preferred_element_type=F32)
        o1 = jnp.dot(hid[1], wb[slot, 1], preferred_element_type=F32)
        g0 = jnp.concatenate([gate[0]] * (nt // TAIL), axis=1)
        g1 = jnp.concatenate([gate[1]] * (nt // TAIL), axis=1)
        cols = pl.ds(pl.multiple_of(n * nt, nt), nt)
        recv[k, :, cols] = (g0 * o0 + g1 * o1).astype(BF)

    def b_copy(k, h, o):
        cy, cx = peer(o)
        cols = pl.ds(h * hw, hw)
        return pltpu.make_async_remote_copy(
            src_ref=recv.at[k, rows_of(cy * 4 + cx), cols], dst_ref=back.at[k, rows_of(me), cols],
            send_sem=b_ssem.at[k, h, o], recv_sem=b_rsem.at[k, h, o],
            device_id=(z, cy, cx), device_id_type=MESH)

    def give_back(k, h):
        for o in order:
            b_copy(k, h, o).start()
        cols = slice(h * hw, h * hw + hw)
        back[k, rows_of(me), cols] = recv[k, rows_of(me), cols]

    def back_wait(k, h):
        for o in order:
            b_copy(k, h, o).wait_recv()

    def s_copy(k, s):
        if k == 1:
            target, slot = src_z[1], jnp.where(z % 2 == 0, z + 1, 4)
        elif k == 2:
            target = z + 1 - 2 * (z // 2)
            slot = jnp.where(z < 2, 2, jnp.where(z == 2, 4, 1))
        else:
            target, slot = z + 1 - 2 * (z // 2), src_z[3]
        cols = pl.ds(s * sw, sw)
        return pltpu.make_async_remote_copy(
            src_ref=zsend.at[k - 1, :, cols], dst_ref=zrecv.at[slot, :, cols],
            send_sem=s_ssem.at[k - 1, s], recv_sem=s_rsem.at[slot, s],
            device_id=(target, ey, ex), device_id_type=MESH)

    def s_wait(slot, s):
        cols = pl.ds(s * sw, sw)
        pltpu.make_async_remote_copy(
            src_ref=zsend.at[0, :, cols], dst_ref=zrecv.at[slot, :, cols],
            send_sem=s_ssem.at[0, s], recv_sem=s_rsem.at[slot, s],
            device_id=(z, ey, ex), device_id_type=MESH).wait_recv()

    def partial(k, s):
        return jnp.dot(unpack[k], back[k, :, s * sw:s * sw + sw], preferred_element_type=F32)

    def slices(h):
        return range(h * per_half, h * per_half + per_half)

    def finish_end(k, h):
        back_wait(k, h)
        for s in slices(h):
            zsend[k - 1, :, s * sw:s * sw + sw] = partial(k, s).astype(BF)
            s_copy(k, s).start()

    def finish_mid(k, h):
        back_wait(k, h)
        for s in slices(h):
            cols = slice(s * sw, s * sw + sw)
            s_wait(src_z[k], s)
            total = partial(k, s) + zrecv[src_z[k], :, cols].astype(F32)
            zsend[k - 1, :, cols] = total.astype(BF)
            s_copy(k, s).start()

    def finish_home(h):
        back_wait(0, h)
        for s in slices(h):
            cols = slice(s * sw, s * sw + sw)

            @pl.when(z > 0)
            def _():
                s_wait(z, s)

            @pl.when(z < 3)
            def _():
                s_wait(4, s)
            total = zbuf[z, :, cols].astype(F32) + partial(0, s)

            @pl.when(z == 0)
            def _():
                y_ref[:, cols] = (total + zrecv[4, :, cols].astype(F32)).astype(BF)

            @pl.when(z == 3)
            def _():
                y_ref[:, cols] = (total + zrecv[3, :, cols].astype(F32)).astype(BF)

            @pl.when(mid)
            def _():
                both = zrecv[z, :, cols].astype(F32) + zrecv[4, :, cols].astype(F32)
                y_ref[:, cols] = (total + both).astype(BF)

    per = 2 * n_f + n_n
    third = 2 * n_f + (n_n + 1) // 2

    def mids_take(k):
        z_wait(k)
        fwd_copy(k).start()

    def first_arrivals():
        z_wait(1)
        forward(1)
        pl.when(mid)(lambda: mids_take(2))
        relay(1)

    def end_relay(k):
        z_wait(k)
        relay(k)

    every = z >= 0
    events = (
        (2, every, first_arrivals),
        (per - 1, mid, lambda: relay(2)),
        (per, every, lambda: arrive(1)),
        (per + 2, end, lambda: end_relay(2)),
        (per + 2, mid, lambda: mids_take(3)),
        (per + 4, mid, lambda: relay(3)),
        (per + third, every, lambda: give_back(1, 0)),
        (2 * per, every, lambda: arrive(2)),
        (2 * per + 2, end, lambda: end_relay(3)),
        (2 * per + 3, every, lambda: give_back(1, 1)),
        (2 * per + 4, end, lambda: finish_end(1, 0)),
        (2 * per + third, every, lambda: give_back(2, 0)),
        (3 * per, mid, lambda: give_back(2, 1)),
        (3 * per, every, lambda: arrive(3)),
        (3 * per + 4, end, lambda: finish_end(1, 1)),
        (3 * per + third - 1, end, lambda: finish_end(2, 0)),
        (3 * per + third, every, lambda: give_back(3, 0)),
    )

    relay(0)
    arrive(0)

    def step(t, carry):
        for when, cond, act in events:
            pl.when(jnp.logical_and(t == when, cond))(act)
        k, i = t // per, t % per

        @pl.when(i == 2 * n_f)
        def _():
            step_gate(k)

        @pl.when(i < 2 * n_f)
        def _():
            step_a(k, i)

        @pl.when(i >= 2 * n_f)
        def _():
            step_b(k, i - 2 * n_f)
        return carry
    lax.fori_loop(0, ZED * per, step, 0)

    give_back(3, 1)
    pl.when(end)(lambda: give_back(2, 1))
    give_back(0, 0)
    give_back(0, 1)

    @pl.when(end)
    def _():
        finish_end(3, 0)
        finish_end(3, 1)
        finish_end(2, 1)

    @pl.when(mid)
    def _():
        finish_mid(2, 0)
        finish_mid(3, 0)
        finish_mid(1, 0)
        finish_mid(3, 1)
        finish_mid(1, 1)
        finish_mid(2, 1)
    for h in range(HALVES):
        finish_home(h)

    @pl.when(z > 0)
    def _():
        z_copy(z, z - 1, 0).wait_send()

    @pl.when(z < 3)
    def _():
        z_copy(z, z + 1, 1).wait_send()

    @pl.when(mid)
    def _():
        for k in range(1, ZED):
            fwd_copy(k).wait_send()
    for k in range(ZED):
        for o in order:
            d_copy(k, o).wait_send()
            for h in range(HALVES):
                b_copy(k, h, o).wait_send()
    for k in range(1, ZED):
        for s in range(SLICES):
            s_copy(k, s).wait_send()


def split_gates(gates):
    first = lax.reduce_precision(gates, 8, 7)
    second = lax.reduce_precision(gates - first, 8, 7)
    third = gates - first - second
    return first, second, third


def solution(mesh):
    ep_axes = tuple(mesh.axis_names)
    num_devices = math.prod(mesh.shape[a] for a in ep_axes)
    row_spec = P(ep_axes, None)
    w_spec = P(ep_axes, None, None)

    def local_layer(tokens, expert_ids, gate_weights, w_gate, w_up, w_down):
        tok, wide = tokens.shape
        ff = w_gate.shape[2]
        cap = tok * expert_ids.shape[1] // num_devices
        rows = PLANE * cap
        ft, nt = FT, NT
        full = wide + TAIL

        def eight(v):
            return jnp.pad(v.astype(F32), ((0, 0), (0, 2)), constant_values=-1.0)
        parts = [eight(expert_ids // 2), eight(expert_ids)]
        parts += [eight(g) for g in split_gates(gate_weights)]
        tail = jnp.concatenate(parts, axis=1)
        tail = jnp.pad(tail, ((0, 0), (0, TAIL - tail.shape[1]))).astype(BF)

        dims = (tok, wide, ff, cap, ft, nt)
        vm = pl.BlockSpec(memory_space=pltpu.VMEM)
        hbm = pl.BlockSpec(memory_space=pl.ANY)
        dma = pltpu.SemaphoreType.DMA
        return pl.pallas_call(
            functools.partial(layer_kernel, dims),
            out_shape=jax.ShapeDtypeStruct((tok, wide), BF),
            in_specs=[hbm, vm, hbm, hbm, hbm],
            out_specs=vm,
            scratch_shapes=[
                pltpu.VMEM((ZED, tok, full), BF),
                pltpu.VMEM((ZED, rows, full), BF),
                pltpu.VMEM((ZED, rows, full), BF),
                pltpu.VMEM((ZED, rows, wide), BF),
                pltpu.VMEM((2, rows, ff), BF),
                pltpu.VMEM((2, rows, TAIL), F32),
                pltpu.VMEM((ZED - 1, tok, wide), BF),
                pltpu.VMEM((ZED + 1, tok, wide), BF),
                pltpu.VMEM((ZED, tok, rows), BF),
                pltpu.VMEM((2, 2, wide, ft), BF),
                pltpu.VMEM((2, 2, ff, nt), BF),
                dma((1,)), dma((2, 2)), dma((2, 2)),
                dma((5,)), dma((ZED,)),
                dma((ZED, PLANE)), dma((ZED, PLANE)),
                dma((ZED, HALVES, PLANE)), dma((ZED, HALVES, PLANE)),
                dma((ZED - 1, SLICES)), dma((ZED + 1, SLICES)),
            ],
            compiler_params=pltpu.CompilerParams(
                collective_id=0, has_side_effects=True, vmem_limit_bytes=67_000_000),
            name="moe_layer",
        )(tokens, tail, w_gate, w_up, w_down)

    return jax.shard_map(local_layer, mesh=mesh, in_specs=(row_spec, row_spec, row_spec, w_spec, w_spec, w_spec), out_specs=row_spec, check_vma=False)
```

```python
import functools
import math
import jax
import jax.numpy as jnp
from jax import lax
from jax.experimental import pallas as pl
from jax.experimental.pallas import tpu as pltpu
from jax.sharding import PartitionSpec as P

BF = jnp.bfloat16
F32 = jnp.float32
MESH = pl.DeviceIdType.MESH
TAIL = 128
PLANE = 8
ZED = 4
SLICES = 10
HALVES = 2
FIRST = 6
EARLY = 3
FT = 512
NT = 512


def layer_kernel(dims, x_ref, ids_ref, g_ref, w1_ref, w3_ref, w2_ref, y_ref,
                 zbuf, send, recv, back, hid, gate, zsend, zrecv, unpack, pick, meta, y_buf, wa, wb,
                 x_sem, y_sem, wa_sem, wb_sem, z_ssem, z_rsem, d_ssem, d_rsem,
                 b_ssem, b_rsem, s_ssem, s_rsem):
    tok, wide, ff, cap, ft, nt = dims
    rows = PLANE * cap
    full = wide + TAIL
    sw = wide // SLICES
    starts = (0, FIRST * sw, wide)
    n_f, n_n = ff // ft, wide // nt
    z = lax.axis_index("ez")
    ey = lax.axis_index("ey")
    ex = lax.axis_index("ex")
    me = ey * 4 + ex
    mid = jnp.logical_and(z > 0, z < 3)
    end = jnp.logical_or(z < 1, z > 2)

    def peer(o):
        cy = ey if o < 4 else 1 - ey
        cx = (ex, ex + 1 - 2 * (ex % 2), (ex + 2) % 4, 3 - ex)[o % 4]
        return cy, cx

    def rows_of(q):
        return pl.ds(pl.multiple_of(q * cap, cap), cap)

    src_z = (z, z + 1 - 2 * (z % 2), 2 - z // 2, 3 - 3 * (z // 2))
    order = (6, 4, 2, 7, 5, 3, 1)
    others = pl.ds(0, (PLANE - 1) * cap)

    def slices(h, k=0):
        cut = EARLY if k == 1 else FIRST
        return range(0, cut) if h == 0 else range(cut, SLICES)

    def hidden(h, off=0):
        return pl.ds(off + starts[h], starts[h + 1] - starts[h])

    def half(h):
        return pl.ds(0, TAIL + starts[1]) if h == 0 else hidden(1, TAIL)

    barrier = pltpu.get_barrier_semaphore()
    for o in range(1, PLANE):
        cy, cx = peer(o)
        pl.semaphore_signal(barrier, inc=1, device_id=(z, cy, cx), device_id_type=MESH)

    @pl.when(z > 0)
    def _():
        pl.semaphore_signal(barrier, inc=1, device_id=(z - 1, ey, ex), device_id_type=MESH)

    @pl.when(z < 3)
    def _():
        pl.semaphore_signal(barrier, inc=1, device_id=(z + 1, ey, ex), device_id_type=MESH)

    own = pltpu.make_async_copy(x_ref, zbuf.at[z, :, pl.ds(TAIL, wide)], x_sem.at[0])
    own.start()
    ids = ids_ref[...]
    top_k = ids.shape[0]
    first = g_ref[...].astype(BF).astype(F32)
    rest = g_ref[...] - first
    second = rest.astype(BF).astype(F32)
    meta[...] = jnp.zeros_like(meta)
    terms = (lax.shift_right_logical(ids, 1).astype(F32), ids.astype(F32), first, second, rest - second)
    for n, term in enumerate(terms):
        meta[8 * n:8 * n + top_k, :] = term
    zbuf[z, :, :TAIL] = jnp.transpose(meta[...]).astype(BF)

    def a_copies(i):
        l, f, slot = i // n_f, i % n_f, i % 2
        cols = pl.ds(pl.multiple_of(f * ft, ft), ft)
        return [pltpu.make_async_copy(w.at[l, :, cols], wa.at[slot, j], wa_sem.at[slot, j])
                for j, w in enumerate((w1_ref, w3_ref))]

    def b_copies(n):
        slot = n % 2
        cols = pl.ds(pl.multiple_of(n * nt, nt), nt)
        return [pltpu.make_async_copy(w2_ref.at[l, :, cols], wb.at[slot, l], wb_sem.at[slot, l])
                for l in range(2)]

    own.wait()
    pl.semaphore_wait(barrier, PLANE - 1 + jnp.where(mid, 2, 1))

    def z_copy(block, target, i, h):
        return pltpu.make_async_remote_copy(
            src_ref=zbuf.at[block, :, half(h)], dst_ref=zbuf.at[block, :, half(h)],
            send_sem=z_ssem.at[i, h], recv_sem=z_rsem.at[block, h],
            device_id=(target, ey, ex), device_id_type=MESH)

    @pl.when(z > 0)
    def _():
        for h in range(HALVES):
            z_copy(z, z - 1, 0, h).start()

    @pl.when(z < 3)
    def _():
        for h in range(HALVES):
            z_copy(z, z + 1, 1, h).start()

    for c in a_copies(0):
        c.start()

    def fwd_copy(k, h):
        return z_copy(src_z[k], 3 - z if k == 1 else 3 * (z - 1), 1 + k, h)

    def z_wait(k, h):
        z_copy(src_z[k], z, 0, h).wait_recv()

    def d_copy(k, h, o):
        cy, cx = peer(o)
        return pltpu.make_async_remote_copy(
            src_ref=send.at[k, rows_of(cy * 4 + cx), half(h)], dst_ref=recv.at[k, rows_of(me), half(h)],
            send_sem=d_ssem.at[k], recv_sem=d_rsem.at[k, h],
            device_id=(z, cy, cx), device_id_type=MESH)

    def route(k):
        b = src_z[k]
        tail = zbuf[b, :, :TAIL].astype(F32)
        lane = lax.broadcasted_iota(jnp.int32, (tok, TAIL), 1)
        want_dev = jnp.where(lane < PLANE, z * PLANE + lane, -2).astype(F32)
        want_exp = jnp.where(lane < 48, z * 16 + jnp.bitwise_and(lane, 15), -2).astype(F32)
        hit = jnp.zeros((tok, TAIL), F32)
        gates = jnp.zeros((tok, TAIL), F32)
        for j in range(6):
            hit = jnp.where(tail[:, j:j + 1] == want_dev, 1.0, hit)
            part = jnp.where(lane < 16, tail[:, 16 + j:17 + j],
                             jnp.where(lane < 32, tail[:, 24 + j:25 + j], tail[:, 32 + j:33 + j]))
            gates = jnp.where(tail[:, 8 + j:9 + j] == want_exp, part, gates)
        r_i = lax.broadcasted_iota(jnp.int32, (tok, tok), 0)
        c_i = lax.broadcasted_iota(jnp.int32, (tok, tok), 1)
        tri = jnp.where(c_i <= r_i, 1.0, 0.0).astype(BF)
        rank = jnp.dot(tri, hit.astype(BF), preferred_element_type=F32)
        pos = jnp.where(hit > 0.0, rank, 0.0).astype(BF)
        d_i = lax.broadcasted_iota(jnp.int32, (TAIL, rows), 0)
        s_i = lax.broadcasted_iota(jnp.int32, (TAIL, rows), 1)
        spread = jnp.where(jnp.logical_and(s_i >= d_i * cap, s_i < d_i * cap + cap), 1.0, 0.0).astype(BF)
        l_i = lax.broadcasted_iota(jnp.int32, (tok, rows), 1)
        slot_l = l_i + 1
        for q in range(1, PLANE):
            slot_l = slot_l - jnp.where(l_i >= q * cap, cap, 0)
        at_l = jnp.dot(pos, spread, preferred_element_type=F32)
        unpack[k] = jnp.where(at_l == slot_l.astype(F32), 1.0, 0.0).astype(BF)
        d_t = lax.broadcasted_iota(jnp.int32, (rows, TAIL), 1)
        s_t = lax.broadcasted_iota(jnp.int32, (rows, TAIL), 0)
        spread_t = jnp.where(jnp.logical_and(s_t >= d_t * cap, s_t < d_t * cap + cap), 1.0, 0.0).astype(BF)
        r_t = lax.broadcasted_iota(jnp.int32, (rows, tok), 0)
        slot_r = r_t + 1
        for q in range(1, PLANE):
            slot_r = slot_r - jnp.where(r_t >= q * cap, cap, 0)
        at_r = lax.dot_general(spread_t, pos, (((1,), (1,)), ((), ())), preferred_element_type=F32)
        pick[...] = jnp.where(at_r == slot_r.astype(F32), 1.0, 0.0).astype(BF)
        send[k, :, :TAIL] = jnp.dot(pick[...], gates.astype(BF), preferred_element_type=F32).astype(BF)

    def relay(k, h):
        if h == 0:
            route(k)
        for s in slices(h):
            cols = slice(TAIL + s * sw, TAIL + s * sw + sw)
            send[k, :, cols] = jnp.dot(pick[...], zbuf[src_z[k], :, cols], preferred_element_type=F32).astype(BF)
        for o in order:
            d_copy(k, h, o).start()
        recv[k, rows_of(me), half(h)] = send[k, rows_of(me), half(h)]

    def arrive(k):
        for h in range(HALVES):
            pltpu.make_async_remote_copy(
                src_ref=send.at[k, others, half(h)], dst_ref=recv.at[k, others, half(h)],
                send_sem=d_ssem.at[k], recv_sem=d_rsem.at[k, h],
                device_id=(z, ey, ex), device_id_type=MESH).wait_recv()

    def step_a(k, i):
        @pl.when(i + 1 < 2 * n_f)
        def _():
            for c in a_copies(i + 1):
                c.start()

        @pl.when(i + 1 == 2 * n_f)
        def _():
            for c in b_copies(0):
                c.start()
        for c in a_copies(i):
            c.wait()
        slot = i % 2
        x = recv[k, :, TAIL:]
        a = jnp.dot(x, wa[slot, 0], preferred_element_type=F32)
        b = jnp.dot(x, wa[slot, 1], preferred_element_type=F32)
        cols = pl.ds(pl.multiple_of((i % n_f) * ft, ft), ft)
        hid[i // n_f, :, cols] = (jax.nn.silu(a) * b).astype(BF)

    def step_gate(k):
        tail = recv[k, :, :TAIL].astype(F32)
        lane = lax.broadcasted_iota(jnp.int32, (rows, TAIL), 1)
        for l in range(2):
            at = jnp.where(lane < 48, jnp.bitwise_and(lane, 15), -1) == me * 2 + l
            g = jnp.sum(jnp.where(at, tail, 0.0), axis=1, keepdims=True)
            gate[l] = jnp.broadcast_to(g, (rows, TAIL))

    def step_b(k, n):
        @pl.when(n + 1 < n_n)
        def _():
            for c in b_copies(n + 1):
                c.start()

        @pl.when(jnp.logical_and(n + 1 == n_n, k < ZED - 1))
        def _():
            for c in a_copies(0):
                c.start()
        for c in b_copies(n):
            c.wait()
        slot = n % 2
        o0 = jnp.dot(hid[0], wb[slot, 0], preferred_element_type=F32)
        o1 = jnp.dot(hid[1], wb[slot, 1], preferred_element_type=F32)
        g0 = jnp.concatenate([gate[0]] * (nt // TAIL), axis=1)
        g1 = jnp.concatenate([gate[1]] * (nt // TAIL), axis=1)
        cols = pl.ds(pl.multiple_of(TAIL + n * nt, TAIL), nt)
        recv[k, :, cols] = (g0 * o0 + g1 * o1).astype(BF)

    def back_cols(k, h, off=0):
        part = slices(h, k)
        return pl.ds(off + part[0] * sw, len(part) * sw)

    def b_copy(k, h, rows_there, rows_here, device):
        return pltpu.make_async_remote_copy(
            src_ref=recv.at[k, rows_there, back_cols(k, h, TAIL)], dst_ref=back.at[k, rows_here, back_cols(k, h)],
            send_sem=b_ssem.at[k], recv_sem=b_rsem.at[k, h],
            device_id=device, device_id_type=MESH)

    def give_back(k, h, peers=order):
        for o in peers:
            cy, cx = peer(o)
            b_copy(k, h, rows_of(cy * 4 + cx), rows_of(me), (z, cy, cx)).start()
        if order[-1] in peers:
            back[k, rows_of(me), back_cols(k, h)] = recv[k, rows_of(me), back_cols(k, h, TAIL)]

    def back_wait(k, h):
        b_copy(k, h, others, others, (z, ey, ex)).wait_recv()

    def s_copy(k, s):
        if k == 1:
            target, slot = src_z[1], jnp.where(z % 2 == 0, z + 1, 4)
        elif k == 2:
            target = z + 1 - 2 * (z // 2)
            slot = jnp.where(z < 2, 2, jnp.where(z == 2, 4, 1))
        else:
            target, slot = z + 1 - 2 * (z // 2), src_z[3]
        cols = pl.ds(s * sw, sw)
        return pltpu.make_async_remote_copy(
            src_ref=zsend.at[k - 1, :, cols], dst_ref=zrecv.at[slot, :, cols],
            send_sem=s_ssem.at[k - 1], recv_sem=s_rsem.at[slot, s],
            device_id=(target, ey, ex), device_id_type=MESH)

    def s_wait(slot, s):
        cols = pl.ds(s * sw, sw)
        pltpu.make_async_remote_copy(
            src_ref=zsend.at[0, :, cols], dst_ref=zrecv.at[slot, :, cols],
            send_sem=s_ssem.at[0], recv_sem=s_rsem.at[slot, s],
            device_id=(z, ey, ex), device_id_type=MESH).wait_recv()

    def partial(k, s):
        return jnp.dot(unpack[k], back[k, :, s * sw:s * sw + sw], preferred_element_type=F32)

    def finish_end(k, some):
        for s in some:
            zsend[k - 1, :, s * sw:s * sw + sw] = partial(k, s).astype(BF)
            s_copy(k, s).start()

    def finish_mid(k, some):
        for s in some:
            cols = slice(s * sw, s * sw + sw)
            s_wait(src_z[k], s)
            total = partial(k, s) + zrecv[src_z[k], :, cols].astype(F32)
            zsend[k - 1, :, cols] = total.astype(BF)
            s_copy(k, s).start()

    def y_copy(s):
        cols = pl.ds(s * sw, sw)
        return pltpu.make_async_copy(y_buf.at[:, cols], y_ref.at[:, cols], y_sem.at[0])

    def finish_home(h):
        back_wait(0, h)
        for s in slices(h):
            cols = slice(s * sw, s * sw + sw)

            @pl.when(z > 0)
            def _():
                s_wait(z, s)

            @pl.when(z < 3)
            def _():
                s_wait(4, s)
            x = zbuf[z, :, TAIL + s * sw:TAIL + s * sw + sw].astype(F32)
            total = x + partial(0, s)

            @pl.when(z == 0)
            def _():
                y_buf[:, cols] = (total + zrecv[4, :, cols].astype(F32)).astype(BF)

            @pl.when(z == 3)
            def _():
                y_buf[:, cols] = (total + zrecv[3, :, cols].astype(F32)).astype(BF)

            @pl.when(mid)
            def _():
                both = zrecv[z, :, cols].astype(F32) + zrecv[4, :, cols].astype(F32)
                y_buf[:, cols] = (total + both).astype(BF)
            y_copy(s).start()

    per = 2 * n_f + n_n
    third = 2 * n_f + (n_n + 1) // 2

    def take(k, h):
        z_wait(k, h)
        fwd_copy(k, h).start()

    def mids_take(*which):
        @pl.when(mid)
        def _():
            for k, h in which:
                take(k, h)

    def ends_take(k, h):
        pl.when(end)(lambda: z_wait(k, h))

    def at_start():
        relay(0, 0)
        relay(0, 1)
        ends_take(1, 0)
        mids_take((1, 0), (2, 0))
        relay(1, 0)
        arrive(0)

    def take_1_1():
        ends_take(1, 1)
        mids_take((1, 1), (2, 1))
        relay(1, 1)

    def take_2_0():
        ends_take(2, 0)
        relay(2, 0)

    def take_2_1():
        ends_take(2, 1)
        relay(2, 1)
        mids_take((3, 1),)

    def take_3(h):
        ends_take(3, h)
        relay(3, h)

    def drain_tokens():
        for h in range(HALVES):
            @pl.when(z > 0)
            def _():
                z_copy(z, z - 1, 0, h).wait_send()

            @pl.when(z < 3)
            def _():
                z_copy(z, z + 1, 1, h).wait_send()

            @pl.when(mid)
            def _():
                for k in range(1, ZED):
                    fwd_copy(k, h).wait_send()
        for k in range(ZED):
            pltpu.make_async_remote_copy(
                src_ref=send.at[k, others], dst_ref=recv.at[k, others],
                send_sem=d_ssem.at[k], recv_sem=d_rsem.at[k, 0],
                device_id=(z, ey, ex), device_id_type=MESH).wait_send()

    def drain_rows(k):
        pltpu.make_async_remote_copy(
            src_ref=recv.at[k, others, pl.ds(TAIL, wide)], dst_ref=back.at[k, others],
            send_sem=b_ssem.at[k], recv_sem=b_rsem.at[k, 0],
            device_id=(z, ey, ex), device_id_type=MESH).wait_send()

    def drain_sums(k):
        pltpu.make_async_remote_copy(
            src_ref=zsend.at[k - 1], dst_ref=zrecv.at[0],
            send_sem=s_ssem.at[k - 1], recv_sem=s_rsem.at[0, 0],
            device_id=(z, ey, ex), device_id_type=MESH).wait_send()

    def sum_end(k, h):
        back_wait(k, h)
        finish_end(k, slices(h, k))

    def sum_mid(k, h):
        back_wait(k, h)
        finish_mid(k, slices(h, k))

    every = z >= 0
    events = (
        (3, every, take_1_1),
        (per - 1, every, lambda: give_back(0, 0, (2, 4))),
        (per, every, take_2_0),
        (per, every, lambda: arrive(1)),
        (per + 1, mid, lambda: mids_take((3, 0))),
        (per + 5, every, take_2_1),
        (per + 8, every, lambda: give_back(1, 0)),
        (2 * per, every, lambda: take_3(0)),
        (2 * per, every, lambda: arrive(2)),
        (2 * per + 2, end, lambda: sum_end(1, 0)),
        (2 * per + 4, every, lambda: take_3(1)),
        (2 * per + third, every, lambda: give_back(2, 0)),
        (3 * per, every, lambda: give_back(2, 1)),
        (3 * per, every, lambda: arrive(3)),
        (3 * per + 5, end, lambda: sum_end(2, 0)),
        (3 * per + third, every, lambda: give_back(3, 0)),
        (3 * per + third, end, lambda: sum_end(2, 1)),
        (3 * per + third + 1, mid, lambda: sum_mid(2, 0)),
    )

    at_start()

    def step(t, carry):
        for when, cond, act in events:
            pl.when(jnp.logical_and(t == when, cond))(act)
        k, i = t // per, t % per

        @pl.when(i == 2 * n_f)
        def _():
            step_gate(k)

        @pl.when(i < 2 * n_f)
        def _():
            step_a(k, i)

        @pl.when(i >= 2 * n_f)
        def _():
            step_b(k, i - 2 * n_f)
        return carry
    lax.fori_loop(0, ZED * per, step, 0)

    give_back(3, 1)
    give_back(1, 1)
    give_back(0, 0, (6, 7, 5, 3, 1))
    give_back(0, 1)
    drain_tokens()

    @pl.when(end)
    def _():
        sum_end(3, 0)
        sum_end(3, 1)
        sum_end(1, 1)

    @pl.when(mid)
    def _():
        sum_mid(2, 1)
        sum_mid(3, 0)
        back_wait(1, 0)
        finish_mid(1, slices(0, 1))
        back_wait(1, 1)
        finish_mid(1, range(EARLY, FIRST))
        sum_mid(3, 1)
        finish_mid(1, slices(1))
    for k in range(1, ZED):
        drain_rows(k)
    finish_home(0)
    finish_home(1)
    drain_rows(0)
    for k in range(1, ZED):
        drain_sums(k)
    pltpu.make_async_copy(y_buf, y_ref, y_sem.at[0]).wait()


def solution(mesh):
    ep_axes = tuple(mesh.axis_names)
    num_devices = math.prod(mesh.shape[a] for a in ep_axes)
    row_spec = P(ep_axes, None)
    w_spec = P(ep_axes, None, None)

    def local_layer(tokens, expert_ids, gate_weights, w_gate, w_up, w_down):
        tok, wide = tokens.shape
        ff = w_gate.shape[2]
        cap = tok * expert_ids.shape[1] // num_devices
        rows = PLANE * cap
        ft, nt = FT, NT
        full = wide + TAIL
        dims = (tok, wide, ff, cap, ft, nt)
        vm = pl.BlockSpec(memory_space=pltpu.VMEM)
        hbm = pl.BlockSpec(memory_space=pl.ANY)
        dma = pltpu.SemaphoreType.DMA
        return pl.pallas_call(
            functools.partial(layer_kernel, dims),
            out_shape=jax.ShapeDtypeStruct((tok, wide), BF),
            in_specs=[hbm, vm, vm, hbm, hbm, hbm],
            out_specs=hbm,
            scratch_shapes=[
                pltpu.VMEM((ZED, tok, full), BF),
                pltpu.VMEM((ZED, rows, full), BF),
                pltpu.VMEM((ZED, rows, full), BF),
                pltpu.VMEM((ZED, rows, wide), BF),
                pltpu.VMEM((2, rows, ff), BF),
                pltpu.VMEM((2, rows, TAIL), F32),
                pltpu.VMEM((ZED - 1, tok, wide), BF),
                pltpu.VMEM((ZED + 1, tok, wide), BF),
                pltpu.VMEM((ZED, tok, rows), BF),
                pltpu.VMEM((rows, tok), BF),
                pltpu.VMEM((TAIL, tok), F32),
                pltpu.VMEM((tok, wide), BF),
                pltpu.VMEM((2, 2, wide, ft), BF),
                pltpu.VMEM((2, 2, ff, nt), BF),
                dma((1,)), dma((1,)), dma((2, 2)), dma((2, 2)),
                dma((5, HALVES)), dma((ZED, HALVES)),
                dma((ZED,)), dma((ZED, HALVES)),
                dma((ZED,)), dma((ZED, HALVES)),
                dma((ZED - 1,)), dma((ZED + 1, SLICES)),
            ],
            compiler_params=pltpu.CompilerParams(
                collective_id=0, has_side_effects=True, vmem_limit_bytes=67_000_000),
            name="moe_layer",
        )(tokens, expert_ids.T, gate_weights.T, w_gate, w_up, w_down)

    return jax.shard_map(local_layer, mesh=mesh, in_specs=(row_spec, row_spec, row_spec, w_spec, w_spec, w_spec), out_specs=row_spec, check_vma=False)
```

```python
import functools
import math
import jax
import jax.numpy as jnp
from jax import lax
from jax.experimental import pallas as pl
from jax.experimental.pallas import tpu as pltpu
from jax.sharding import PartitionSpec as P

BF = jnp.bfloat16
F32 = jnp.float32
MESH = pl.DeviceIdType.MESH
TAIL = 128
PLANE = 8
ZED = 4
SLICES = 10
HALVES = 2
FIRST = 6
LAG = 2
CUTS = (0, 3, 6, 10)
FT = 512
NT = 512


def layer_kernel(dims, x_ref, ids_ref, g_ref, w1_ref, w3_ref, w2_ref, y_ref,
                 zbuf, send, recv, back, hid, gate, zsend, zrecv, unpack, pick, meta, y_buf, wa, wb,
                 x_sem, y_sem, wa_sem, wb_sem, z_ssem, z_rsem, d_ssem, d_rsem,
                 b_ssem, b_rsem, s_ssem, s_rsem):
    tok, wide, ff, cap, ft, nt = dims
    rows = PLANE * cap
    full = wide + TAIL
    sw = wide // SLICES
    starts = (0, FIRST * sw, wide)
    n_f, n_n = ff // ft, wide // nt
    z = lax.axis_index("ez")
    ey = lax.axis_index("ey")
    ex = lax.axis_index("ex")
    me = ey * 4 + ex
    mid = jnp.logical_and(z > 0, z < 3)
    end = jnp.logical_or(z < 1, z > 2)

    def peer(o):
        cy = ey if o < 4 else 1 - ey
        cx = (ex, ex + 1 - 2 * (ex % 2), (ex + 2) % 4, 3 - ex)[o % 4]
        return cy, cx

    def rows_of(q):
        return pl.ds(pl.multiple_of(q * cap, cap), cap)

    src_z = (z, z + 1 - 2 * (z % 2), 2 - z // 2, 3 - 3 * (z // 2))
    order = (6, 4, 2, 7, 5, 3, 1)
    others = pl.ds(0, (PLANE - 1) * cap)

    def slices(h):
        return range(0, FIRST) if h == 0 else range(FIRST, SLICES)

    parts = len(CUTS) - 1

    def part(h):
        return range(CUTS[h], CUTS[h + 1])

    def hidden(h, off=0):
        return pl.ds(off + starts[h], starts[h + 1] - starts[h])

    def half(h):
        return pl.ds(0, TAIL + starts[1]) if h == 0 else hidden(1, TAIL)

    barrier = pltpu.get_barrier_semaphore()
    for o in range(1, PLANE):
        cy, cx = peer(o)
        pl.semaphore_signal(barrier, inc=1, device_id=(z, cy, cx), device_id_type=MESH)

    @pl.when(z > 0)
    def _():
        pl.semaphore_signal(barrier, inc=1, device_id=(z - 1, ey, ex), device_id_type=MESH)

    @pl.when(z < 3)
    def _():
        pl.semaphore_signal(barrier, inc=1, device_id=(z + 1, ey, ex), device_id_type=MESH)

    own = pltpu.make_async_copy(x_ref, zbuf.at[z, :, pl.ds(TAIL, wide)], x_sem.at[0])
    own.start()
    ids = ids_ref[...]
    top_k = ids.shape[0]
    first = g_ref[...].astype(BF).astype(F32)
    rest = g_ref[...] - first
    second = rest.astype(BF).astype(F32)
    meta[...] = jnp.zeros_like(meta)
    terms = (lax.shift_right_logical(ids, 1).astype(F32), ids.astype(F32), first, second, rest - second)
    for n, term in enumerate(terms):
        meta[8 * n:8 * n + top_k, :] = term
    zbuf[z, :, :TAIL] = jnp.transpose(meta[...]).astype(BF)

    def a_copies(i):
        l, f, slot = i // n_f, i % n_f, i % 2
        cols = pl.ds(pl.multiple_of(f * ft, ft), ft)
        return [pltpu.make_async_copy(w.at[l, :, cols], wa.at[slot, j], wa_sem.at[slot, j])
                for j, w in enumerate((w1_ref, w3_ref))]

    def b_copies(n):
        slot = n % 2
        cols = pl.ds(pl.multiple_of(n * nt, nt), nt)
        return [pltpu.make_async_copy(w2_ref.at[l, :, cols], wb.at[slot, l], wb_sem.at[slot, l])
                for l in range(2)]

    own.wait()
    pl.semaphore_wait(barrier, PLANE - 1 + jnp.where(mid, 2, 1))

    def z_copy(block, target, i, h):
        return pltpu.make_async_remote_copy(
            src_ref=zbuf.at[block, :, half(h)], dst_ref=zbuf.at[block, :, half(h)],
            send_sem=z_ssem.at[i, h], recv_sem=z_rsem.at[block, h],
            device_id=(target, ey, ex), device_id_type=MESH)

    @pl.when(z > 0)
    def _():
        for h in range(HALVES):
            z_copy(z, z - 1, 0, h).start()

    @pl.when(z < 3)
    def _():
        for h in range(HALVES):
            z_copy(z, z + 1, 1, h).start()

    for c in a_copies(0):
        c.start()

    def fwd_copy(k, h):
        return z_copy(src_z[k], 3 - z if k == 1 else 3 * (z - 1), 1 + k, h)

    def z_wait(k, h):
        z_copy(src_z[k], z, 0, h).wait_recv()

    def d_copy(k, h, o):
        cy, cx = peer(o)
        return pltpu.make_async_remote_copy(
            src_ref=send.at[k, rows_of(cy * 4 + cx), half(h)], dst_ref=recv.at[k, rows_of(me), half(h)],
            send_sem=d_ssem.at[k], recv_sem=d_rsem.at[k, h],
            device_id=(z, cy, cx), device_id_type=MESH)

    def route(k):
        b = src_z[k]
        tail = zbuf[b, :, :TAIL].astype(F32)
        lane = lax.broadcasted_iota(jnp.int32, (tok, TAIL), 1)
        want_dev = jnp.where(lane < PLANE, z * PLANE + lane, -2).astype(F32)
        want_exp = jnp.where(lane < 48, z * 16 + jnp.bitwise_and(lane, 15), -2).astype(F32)
        hit = jnp.zeros((tok, TAIL), F32)
        gates = jnp.zeros((tok, TAIL), F32)
        for j in range(6):
            hit = jnp.where(tail[:, j:j + 1] == want_dev, 1.0, hit)
            part = jnp.where(lane < 16, tail[:, 16 + j:17 + j],
                             jnp.where(lane < 32, tail[:, 24 + j:25 + j], tail[:, 32 + j:33 + j]))
            gates = jnp.where(tail[:, 8 + j:9 + j] == want_exp, part, gates)
        r_i = lax.broadcasted_iota(jnp.int32, (tok, tok), 0)
        c_i = lax.broadcasted_iota(jnp.int32, (tok, tok), 1)
        tri = jnp.where(c_i <= r_i, 1.0, 0.0).astype(BF)
        rank = jnp.dot(tri, hit.astype(BF), preferred_element_type=F32)
        pos = jnp.where(hit > 0.0, rank, 0.0).astype(BF)
        d_i = lax.broadcasted_iota(jnp.int32, (TAIL, rows), 0)
        s_i = lax.broadcasted_iota(jnp.int32, (TAIL, rows), 1)
        spread = jnp.where(jnp.logical_and(s_i >= d_i * cap, s_i < d_i * cap + cap), 1.0, 0.0).astype(BF)
        l_i = lax.broadcasted_iota(jnp.int32, (tok, rows), 1)
        slot_l = l_i + 1
        for q in range(1, PLANE):
            slot_l = slot_l - jnp.where(l_i >= q * cap, cap, 0)
        at_l = jnp.dot(pos, spread, preferred_element_type=F32)
        unpack[k] = jnp.where(at_l == slot_l.astype(F32), 1.0, 0.0).astype(BF)
        d_t = lax.broadcasted_iota(jnp.int32, (rows, TAIL), 1)
        s_t = lax.broadcasted_iota(jnp.int32, (rows, TAIL), 0)
        spread_t = jnp.where(jnp.logical_and(s_t >= d_t * cap, s_t < d_t * cap + cap), 1.0, 0.0).astype(BF)
        r_t = lax.broadcasted_iota(jnp.int32, (rows, tok), 0)
        slot_r = r_t + 1
        for q in range(1, PLANE):
            slot_r = slot_r - jnp.where(r_t >= q * cap, cap, 0)
        at_r = lax.dot_general(spread_t, pos, (((1,), (1,)), ((), ())), preferred_element_type=F32)
        pick[...] = jnp.where(at_r == slot_r.astype(F32), 1.0, 0.0).astype(BF)
        send[k, :, :TAIL] = jnp.dot(pick[...], gates.astype(BF), preferred_element_type=F32).astype(BF)

    def relay(k, h):
        if h == 0:
            route(k)
        for s in slices(h):
            cols = slice(TAIL + s * sw, TAIL + s * sw + sw)
            send[k, :, cols] = jnp.dot(pick[...], zbuf[src_z[k], :, cols], preferred_element_type=F32).astype(BF)
        for o in order:
            d_copy(k, h, o).start()
        recv[k, rows_of(me), half(h)] = send[k, rows_of(me), half(h)]

    def arrive(k):
        for h in range(HALVES):
            pltpu.make_async_remote_copy(
                src_ref=send.at[k, others, half(h)], dst_ref=recv.at[k, others, half(h)],
                send_sem=d_ssem.at[k], recv_sem=d_rsem.at[k, h],
                device_id=(z, ey, ex), device_id_type=MESH).wait_recv()

    def step_a(k, i):
        @pl.when(i + 1 < 2 * n_f)
        def _():
            for c in a_copies(i + 1):
                c.start()

        @pl.when(i + 1 == 2 * n_f)
        def _():
            for c in b_copies(0):
                c.start()
        for c in a_copies(i):
            c.wait()
        slot = i % 2
        x = recv[k, :, TAIL:]
        a = jnp.dot(x, wa[slot, 0], preferred_element_type=F32)
        b = jnp.dot(x, wa[slot, 1], preferred_element_type=F32)
        cols = pl.ds(pl.multiple_of((i % n_f) * ft, ft), ft)
        hid[i // n_f, :, cols] = (jax.nn.silu(a) * b).astype(BF)

    def step_gate(k):
        tail = recv[k, :, :TAIL].astype(F32)
        lane = lax.broadcasted_iota(jnp.int32, (rows, TAIL), 1)
        for l in range(2):
            at = jnp.where(lane < 48, jnp.bitwise_and(lane, 15), -1) == me * 2 + l
            g = jnp.sum(jnp.where(at, tail, 0.0), axis=1, keepdims=True)
            gate[l] = jnp.broadcast_to(g, (rows, TAIL))

    def step_b(k, n):
        @pl.when(n + 1 < n_n)
        def _():
            for c in b_copies(n + 1):
                c.start()

        @pl.when(jnp.logical_and(n + 1 == n_n, k < ZED - 1))
        def _():
            for c in a_copies(0):
                c.start()
        for c in b_copies(n):
            c.wait()
        slot = n % 2
        o0 = jnp.dot(hid[0], wb[slot, 0], preferred_element_type=F32)
        o1 = jnp.dot(hid[1], wb[slot, 1], preferred_element_type=F32)
        g0 = jnp.concatenate([gate[0]] * (nt // TAIL), axis=1)
        g1 = jnp.concatenate([gate[1]] * (nt // TAIL), axis=1)
        cols = pl.ds(pl.multiple_of(TAIL + n * nt, TAIL), nt)
        recv[k, :, cols] = (g0 * o0 + g1 * o1).astype(BF)

    def back_cols(h, off=0):
        return pl.ds(off + CUTS[h] * sw, len(part(h)) * sw)

    def b_copy(k, h, rows_there, rows_here, device):
        return pltpu.make_async_remote_copy(
            src_ref=recv.at[k, rows_there, back_cols(h, TAIL)], dst_ref=back.at[k, rows_here, back_cols(h)],
            send_sem=b_ssem.at[k], recv_sem=b_rsem.at[k, h],
            device_id=device, device_id_type=MESH)

    def give_back(k, h, peers=order):
        for o in peers:
            cy, cx = peer(o)
            b_copy(k, h, rows_of(cy * 4 + cx), rows_of(me), (z, cy, cx)).start()
        if order[-1] in peers:
            back[k, rows_of(me), back_cols(h)] = recv[k, rows_of(me), back_cols(h, TAIL)]

    def back_wait(k, h):
        b_copy(k, h, others, others, (z, ey, ex)).wait_recv()

    def s_copy(k, s):
        if k == 1:
            target, slot = src_z[1], jnp.where(z % 2 == 0, z + 1, 4)
        elif k == 2:
            target = z + 1 - 2 * (z // 2)
            slot = jnp.where(z < 2, 2, jnp.where(z == 2, 4, 1))
        else:
            target, slot = z + 1 - 2 * (z // 2), src_z[3]
        cols = pl.ds(s * sw, sw)
        return pltpu.make_async_remote_copy(
            src_ref=zsend.at[k - 1, :, cols], dst_ref=zrecv.at[slot, :, cols],
            send_sem=s_ssem.at[k - 1], recv_sem=s_rsem.at[slot, s],
            device_id=(target, ey, ex), device_id_type=MESH)

    def s_wait(slot, s):
        cols = pl.ds(s * sw, sw)
        pltpu.make_async_remote_copy(
            src_ref=zsend.at[0, :, cols], dst_ref=zrecv.at[slot, :, cols],
            send_sem=s_ssem.at[0], recv_sem=s_rsem.at[slot, s],
            device_id=(z, ey, ex), device_id_type=MESH).wait_recv()

    def partial(k, s):
        return jnp.dot(unpack[k], back[k, :, s * sw:s * sw + sw], preferred_element_type=F32)

    def finish_end(k, some):
        for s in some:
            zsend[k - 1, :, s * sw:s * sw + sw] = partial(k, s).astype(BF)
            s_copy(k, s).start()

    def finish_mid(k, some):
        for s in some:
            cols = slice(s * sw, s * sw + sw)
            s_wait(src_z[k], s)
            total = partial(k, s) + zrecv[src_z[k], :, cols].astype(F32)
            zsend[k - 1, :, cols] = total.astype(BF)
            s_copy(k, s).start()

    def y_copy(s):
        cols = pl.ds(s * sw, sw)
        return pltpu.make_async_copy(y_buf.at[:, cols], y_ref.at[:, cols], y_sem.at[0])

    def finish_home(h):
        back_wait(0, h)
        for s in part(h):
            cols = slice(s * sw, s * sw + sw)

            @pl.when(z > 0)
            def _():
                s_wait(z, s)

            @pl.when(z < 3)
            def _():
                s_wait(4, s)
            x = zbuf[z, :, TAIL + s * sw:TAIL + s * sw + sw].astype(F32)
            total = x + partial(0, s)

            @pl.when(z == 0)
            def _():
                y_buf[:, cols] = (total + zrecv[4, :, cols].astype(F32)).astype(BF)

            @pl.when(z == 3)
            def _():
                y_buf[:, cols] = (total + zrecv[3, :, cols].astype(F32)).astype(BF)

            @pl.when(mid)
            def _():
                both = zrecv[z, :, cols].astype(F32) + zrecv[4, :, cols].astype(F32)
                y_buf[:, cols] = (total + both).astype(BF)
            y_copy(s).start()

    per = 2 * n_f + n_n
    third = 2 * n_f + (n_n + 1) // 2

    def take(k, h):
        z_wait(k, h)
        fwd_copy(k, h).start()

    def mids_take(*which):
        @pl.when(mid)
        def _():
            for k, h in which:
                take(k, h)

    def ends_take(k, h):
        pl.when(end)(lambda: z_wait(k, h))

    def at_start():
        relay(0, 0)
        relay(0, 1)
        ends_take(1, 0)
        mids_take((1, 0), (2, 0))
        relay(1, 0)
        arrive(0)

    def take_1_1():
        ends_take(1, 1)
        mids_take((1, 1), (2, 1))
        relay(1, 1)

    def take_2_0():
        ends_take(2, 0)
        relay(2, 0)

    def take_2_1():
        ends_take(2, 1)
        relay(2, 1)
        mids_take((3, 1),)

    def take_3(h):
        ends_take(3, h)
        relay(3, h)

    def drain_tokens():
        for h in range(HALVES):
            @pl.when(z > 0)
            def _():
                z_copy(z, z - 1, 0, h).wait_send()

            @pl.when(z < 3)
            def _():
                z_copy(z, z + 1, 1, h).wait_send()

            @pl.when(mid)
            def _():
                for k in range(1, ZED):
                    fwd_copy(k, h).wait_send()
        for k in range(ZED):
            pltpu.make_async_remote_copy(
                src_ref=send.at[k, others], dst_ref=recv.at[k, others],
                send_sem=d_ssem.at[k], recv_sem=d_rsem.at[k, 0],
                device_id=(z, ey, ex), device_id_type=MESH).wait_send()

    def drain_rows(k):
        pltpu.make_async_remote_copy(
            src_ref=recv.at[k, others, pl.ds(TAIL, wide)], dst_ref=back.at[k, others],
            send_sem=b_ssem.at[k], recv_sem=b_rsem.at[k, 0],
            device_id=(z, ey, ex), device_id_type=MESH).wait_send()

    def drain_sums(k):
        pltpu.make_async_remote_copy(
            src_ref=zsend.at[k - 1], dst_ref=zrecv.at[0],
            send_sem=s_ssem.at[k - 1], recv_sem=s_rsem.at[0, 0],
            device_id=(z, ey, ex), device_id_type=MESH).wait_send()

    def sum_end(k, h):
        back_wait(k, h)
        finish_end(k, part(h))

    def sum_mid(k, h):
        back_wait(k, h)
        finish_mid(k, part(h))

    every = z >= 0
    events = (
        (3, every, take_1_1),
        (per - 1, every, lambda: give_back(0, 0, (2, 4))),
        (per - 1, every, lambda: give_back(0, 1, (2, 4))),
        (per, every, take_2_0),
        (per, every, lambda: arrive(1)),
        (per + 1, mid, lambda: mids_take((3, 0))),
        (per + 5, every, take_2_1),
        (2 * per, every, lambda: arrive(2)),
        (2 * per, every, lambda: give_back(1, 0)),
        (2 * per + 2, every, lambda: take_3(0)),
        (2 * per + 3, end, lambda: sum_end(1, 0)),
        (2 * per + 5, every, lambda: take_3(1)),
        (2 * per + third, every, lambda: give_back(2, 0)),
        (2 * per + third + 1, every, lambda: give_back(2, 1)),
        (3 * per, every, lambda: arrive(3)),
        (3 * per, every, lambda: give_back(2, 2)),
        (3 * per + 3, end, lambda: sum_end(2, 0)),
        (3 * per + 6, end, lambda: sum_end(2, 1)),
        (3 * per + third - 1, every, lambda: give_back(3, 0)),
        (3 * per + third, every, lambda: give_back(3, 1)),
        (3 * per + third - 1, mid, lambda: sum_mid(2, 0)),
        (3 * per + third + 1, end, lambda: sum_end(2, 2)),
        (3 * per + third + 1, mid, lambda: sum_mid(2, 1)),
    )

    at_start()

    def step(t, carry):
        for when, cond, act in events:
            pl.when(jnp.logical_and(t == when, cond))(act)
        k, i = t // per, t % per

        @pl.when(i == 2 * n_f)
        def _():
            step_gate(k)

        @pl.when(i < 2 * n_f)
        def _():
            step_a(k, i)

        @pl.when(i >= 2 * n_f)
        def _():
            step_b(k, i - 2 * n_f)
        return carry
    lax.fori_loop(0, ZED * per, step, 0)

    @pl.when(end)
    def _():
        give_back(3, 2)
        give_back(1, 1)
        give_back(1, 2)

    @pl.when(mid)
    def _():
        give_back(1, 1)
        give_back(3, 2)
        give_back(1, 2)
    give_back(0, 0, (6, 7, 5, 3, 1))
    give_back(0, 1, (6, 7, 5, 3, 1))
    give_back(0, 2)
    drain_tokens()

    @pl.when(end)
    def _():
        for h in range(parts):
            sum_end(3, h)
        for h in range(1, parts):
            sum_end(1, h)

    @pl.when(mid)
    def _():
        sum_mid(2, 2)
        for s in range(SLICES + LAG):
            for h in range(parts):
                if s == CUTS[h]:
                    back_wait(3, h)
                if s - LAG == CUTS[h]:
                    back_wait(1, h)
            if s < SLICES:
                finish_mid(3, (s,))
            if s >= LAG:
                finish_mid(1, (s - LAG,))
    for k in range(1, ZED):
        drain_rows(k)
    for h in range(parts):
        finish_home(h)
    drain_rows(0)
    for k in range(1, ZED):
        drain_sums(k)
    pltpu.make_async_copy(y_buf, y_ref, y_sem.at[0]).wait()


def solution(mesh):
    ep_axes = tuple(mesh.axis_names)
    num_devices = math.prod(mesh.shape[a] for a in ep_axes)
    row_spec = P(ep_axes, None)
    w_spec = P(ep_axes, None, None)

    def local_layer(tokens, expert_ids, gate_weights, w_gate, w_up, w_down):
        tok, wide = tokens.shape
        ff = w_gate.shape[2]
        cap = tok * expert_ids.shape[1] // num_devices
        rows = PLANE * cap
        ft, nt = FT, NT
        full = wide + TAIL
        dims = (tok, wide, ff, cap, ft, nt)
        vm = pl.BlockSpec(memory_space=pltpu.VMEM)
        hbm = pl.BlockSpec(memory_space=pl.ANY)
        dma = pltpu.SemaphoreType.DMA
        return pl.pallas_call(
            functools.partial(layer_kernel, dims),
            out_shape=jax.ShapeDtypeStruct((tok, wide), BF),
            in_specs=[hbm, vm, vm, hbm, hbm, hbm],
            out_specs=hbm,
            scratch_shapes=[
                pltpu.VMEM((ZED, tok, full), BF),
                pltpu.VMEM((ZED, rows, full), BF),
                pltpu.VMEM((ZED, rows, full), BF),
                pltpu.VMEM((ZED, rows, wide), BF),
                pltpu.VMEM((2, rows, ff), BF),
                pltpu.VMEM((2, rows, TAIL), F32),
                pltpu.VMEM((ZED - 1, tok, wide), BF),
                pltpu.VMEM((ZED + 1, tok, wide), BF),
                pltpu.VMEM((ZED, tok, rows), BF),
                pltpu.VMEM((rows, tok), BF),
                pltpu.VMEM((TAIL, tok), F32),
                pltpu.VMEM((tok, wide), BF),
                pltpu.VMEM((2, 2, wide, ft), BF),
                pltpu.VMEM((2, 2, ff, nt), BF),
                dma((1,)), dma((1,)), dma((2, 2)), dma((2, 2)),
                dma((5, HALVES)), dma((ZED, HALVES)),
                dma((ZED,)), dma((ZED, HALVES)),
                dma((ZED,)), dma((ZED, len(CUTS) - 1)),
                dma((ZED - 1,)), dma((ZED + 1, SLICES)),
            ],
            compiler_params=pltpu.CompilerParams(
                collective_id=0, has_side_effects=True, vmem_limit_bytes=67_000_000),
            name="moe_layer",
        )(tokens, expert_ids.T, gate_weights.T, w_gate, w_up, w_down)

    return jax.shard_map(local_layer, mesh=mesh, in_specs=(row_spec, row_spec, row_spec, w_spec, w_spec, w_spec), out_specs=row_spec, check_vma=False)
```
